32 devices in a mesh: dp: 1 (over z), ri: 4 (over y), co: 4 (over x), ro: 2 (over core).
Axes of the slice: x: 4, y: 4, z: 1, core: 2. Of those that a mesh axis runs over, the one named last changes fastest.
The devices are a block of a 4x4x8 slice.
Arguments:
- a_mat: bfloat16 [3072, 16384], P(('dp', 'ri', 'ro'), 'co')
- b_mat: bfloat16 [16384, 24576], P(('dp', 'ri', 'ro'), 'co')
Outputs:
- output: bfloat16 [3072, 24576], P(('dp', 'ri', 'ro'), 'co')
All inputs are finite; a program needn't handle non-finite values.
Results may differ from the reference program's by a relative error of at most 0.001.
Values are sent between devices in bfloat16 or wider.
A program may use at most 768 MiB of HBM per device.

```python
import jax
import jax.numpy as jnp

M_ROWS = 3072
N_COLS = 24576
K_DEPTH = 16384


def setup_inputs(seed: int = 0, part: int = 0) -> dict:
    base_key = jax.random.fold_in(jax.random.key(seed), part)
    key_a, key_b = jax.random.split(base_key)
    left_mat = jax.random.normal(key_a, (M_ROWS, K_DEPTH), jnp.float32)
    right_mat = jax.random.normal(key_b, (K_DEPTH, N_COLS), jnp.float32) * (K_DEPTH ** -0.5)
    return {"a_mat": left_mat.astype(jnp.bfloat16), "b_mat": right_mat.astype(jnp.bfloat16)}


def reference(a_mat, b_mat):
    product = jnp.dot(a_mat, b_mat, preferred_element_type=jnp.float32)
    return product.astype(jnp.bfloat16)
```

```python
import functools

import jax
import jax.numpy as jnp
from jax import lax
from jax.experimental import pallas as pl
from jax.experimental.pallas import tpu as pltpu
from jax.sharding import PartitionSpec as P

MESH = pl.DeviceIdType.MESH
NT = 6
F32 = jnp.float32


def kernel(
    ny, nx, a_ref, b_ref, c_ref, bx, s1, ra,
    af, bt, sa, sb, rb, rc, rat, ct,
    bx_send, bx_recv, bt_sem, s1_send, s1_recv, s2_send, s2_recv, s3_send, s3_recv, s4_send, s4_recv,
    a_send, a_recv, b_send, b_recv, c_send, c_recv, ra_sem, ct_sem,
):
    y, x, core = lax.axis_index("ri"), lax.axis_index("co"), lax.axis_index("ro")
    rows = a_ref.shape[0]
    kh = b_ref.shape[0]
    w = b_ref.shape[1] // (2 * NT)
    q = rows // nx
    hq = q // 2

    def ym(d):
        return lax.rem(y + d + ny, ny)

    def xm(d):
        return lax.rem(x + d + nx, nx)

    def quarter(i):
        return pl.ds(pl.multiple_of(i * q, q), q)

    def rcopy(src, dst, ss, rs, **dev):
        return pltpu.make_async_remote_copy(
            src_ref=src, dst_ref=dst, send_sem=ss, recv_sem=rs, device_id=dev, device_id_type=MESH
        )

    barrier = pltpu.get_barrier_semaphore()
    for d in range(1, nx):
        pl.semaphore_signal(barrier, inc=1, device_id={"co": xm(d)}, device_id_type=MESH)
    for d in range(1, ny):
        pl.semaphore_signal(barrier, inc=1, device_id={"ri": ym(d)}, device_id_type=MESH)
    pl.semaphore_signal(barrier, inc=1, device_id={"ro": 1 - core}, device_id_type=MESH)
    pl.semaphore_wait(barrier, nx + ny - 1)

    def s1_copy(d):
        return rcopy(a_ref.at[quarter(xm(d))], s1.at[x], s1_send.at[d], s1_recv.at[x], co=xm(d))

    def s1_start():
        for d in (2, 1, 3):
            s1_copy(d).start()

    odd = lax.rem(x + y, 2) == 1

    @pl.when(odd)
    def _():
        s1_start()

    def cols(tile):
        return pl.ds(pl.multiple_of(tile * w, w), w)

    def bx_copy(tile):
        return rcopy(b_ref.at[:, cols(tile)], bx.at[:, cols(tile)], bx_send.at[tile], bx_recv.at[tile], ro=1 - core)

    def tile_a(t):
        return (1 - lax.rem(t, 2)) * NT + t // 2

    def tile_b(t):
        return lax.rem(t, 2) * NT + t // 2

    def bx_start(t, _):
        bx_copy(tile_a(t)).start()
        return 0

    lax.fori_loop(0, 2 * NT, bx_start, 0)

    def bt_copies(tile, slot):
        return (
            pltpu.make_async_copy(
                b_ref.at[:, cols(tile)], bt.at[slot, pl.ds(pl.multiple_of(core * kh, kh), kh)], bt_sem.at[slot, 0]
            ),
            pltpu.make_async_copy(
                bx.at[:, cols(tile)], bt.at[slot, pl.ds(pl.multiple_of((1 - core) * kh, kh), kh)], bt_sem.at[slot, 1]
            ),
        )

    def bt_start(tile, slot):
        for cp in bt_copies(tile, slot):
            cp.start()

    def bt_wait(tile, slot):
        for cp in bt_copies(tile, slot):
            cp.wait()

    def s2_piece(r, start):
        a = ym(r)
        here = a == x
        for src, cond in ((a_ref.at[quarter(x)], here), (s1.at[a], jnp.logical_not(here))):

            @pl.when(cond)
            def _(src=src):
                dst = af.at[y, quarter(x)]
                if r == 0:
                    cp = pltpu.make_async_copy(src, dst, s2_send.at[0])
                else:
                    cp = rcopy(src, dst, s2_send.at[r], s2_recv.at[y], ri=a)
                if start:
                    cp.start()
                elif r == 0:
                    cp.wait()
                else:
                    cp.wait_send()

    def s1_wait(r):
        a = ym(r)

        @pl.when(a != x)
        def _():
            rcopy(s1.at[a], s1.at[a], s1_send.at[0], s1_recv.at[a], co=a).wait_recv()

    def s2_wait(m):
        rcopy(af.at[m, quarter(x)], af.at[m, quarter(x)], s2_send.at[1], s2_recv.at[m], ri=m).wait_recv()

    def s3_copy(m, side):
        return rcopy(
            af.at[m, quarter(x)], af.at[m, quarter(x)], s3_send.at[m, side], s3_recv.at[m, side], co=xm(1 - 2 * side)
        )

    def half(i, side):
        return pl.ds(pl.multiple_of(i * q + side * hq, hq), hq)

    def s4_copy(m, side):
        part = af.at[m, half(xm(2 * side - 1), side)]
        return rcopy(part, part, s4_send.at[m, side], s4_recv.at[m, side], co=xm(1 - 2 * side))

    def s3_start(m):
        for side in range(2):
            s3_copy(m, side).start()

    def s3_recv_and_relay(m):
        for side in range(2):
            part = af.at[m, quarter(xm(2 * side - 1))]
            rcopy(part, part, s3_send.at[m, side], s3_recv.at[m, side], co=x).wait_recv()
            s4_copy(m, side).start()

    def s4_wait(m):
        for side in range(2):
            part = af.at[m, half(xm(2), side)]
            rcopy(part, part, s4_send.at[m, side], s4_recv.at[m, side], co=x).wait_recv()

    for r in (1, ny - 1):
        s1_wait(r)
        s2_piece(r, True)

    @pl.when(x == ym(2))
    def _():
        s1_start()

    for t in range(2):
        bx_copy(tile_a(t)).wait_recv()
    bt_start(tile_a(0), 0)
    for d in (1, ny - 1):
        s2_wait(ym(d))
        s3_start(ym(d))

    @pl.when(x == y)
    def _():
        s1_start()

    def dest(d):
        return lax.rem(y + 1 + d * (ny - 2), ny)

    def a_copy(d, k, i):
        return rcopy(
            sa.at[d, k, quarter(i)], ra.at[d, k, quarter(i)], a_send.at[d, k, i], a_recv.at[d, k, i], ri=dest(d)
        )

    def b_copy(d, k):
        return rcopy(sb.at[d, k], rb.at[d, k], b_send.at[d, k], b_recv.at[d, k], ri=dest(d))

    def c_copy(d, k):
        return rcopy(sa.at[d, k], rc.at[d, k], c_send.at[d, k], c_recv.at[d, k], ri=dest(d))

    last = 2 * NT - 1

    def run(this, nxt, work, before_next=None):
        def step(t, carry):
            slot = lax.rem(t, 2)

            @pl.when(t < last)
            def _():
                if before_next is not None:
                    before_next(t + 1)
                bt_start(this(t + 1), 1 - slot)

            if nxt is not None:

                @pl.when(t == last)
                def _():
                    bt_start(nxt(0), 1 - slot)

            bt_wait(this(t), slot)
            work(t, lax.rem(t, 2), t // 2, slot)
            return carry

        lax.fori_loop(0, 2 * NT, step, 0)

    def quarter_pass(j, nxt, before_next=None):
        i = xm(j)

        def work(t, d, k, slot):
            sa[d, k, quarter(i)] = jnp.dot(af[dest(d), quarter(i)], bt[slot], preferred_element_type=F32)
            a_copy(d, k, i).start()

        run(tile_a, nxt, work, before_next)

    def wait_bx(t):
        @pl.when(t >= 2)
        def _():
            bx_copy(tile_a(t)).wait_recv()

    quarter_pass(0, tile_a, wait_bx)
    s1_wait(2)
    s2_piece(2, True)
    for d in (1, ny - 1):
        s3_recv_and_relay(ym(d))
    quarter_pass(1, tile_a)
    s2_wait(ym(2))
    s3_start(ym(2))
    s1_wait(0)
    s2_piece(0, True)
    quarter_pass(nx - 1, tile_a)
    for d in (1, ny - 1):
        s4_wait(ym(d))
    s2_piece(0, False)
    s3_start(y)
    s3_recv_and_relay(ym(2))
    quarter_pass(2, tile_b)
    s4_wait(ym(2))
    s3_recv_and_relay(y)

    def b_work(t, d, k, slot):
        sb[d, k] = jnp.dot(af[ym(2)], bt[slot], preferred_element_type=F32)
        b_copy(d, k).start()

    run(tile_b, tile_b, b_work)
    s4_wait(y)

    def c_work(t, d, k, slot):
        for i in range(nx):
            a_copy(d, k, i).wait_send()
        b_copy(d, k).wait_recv()
        sa[d, k] = jnp.dot(af[dest(d)], bt[slot], preferred_element_type=F32) + rb[d, k]
        c_copy(d, k).start()

    run(tile_b, tile_b, c_work)

    def ra_copy(d, k, slot):
        return pltpu.make_async_copy(ra.at[1 - d, k], rat.at[slot], ra_sem.at[slot])

    def ra_start(d, k, slot):
        for i in range(nx):
            a_copy(1 - d, k, i).wait_recv()
        ra_copy(d, k, slot).start()

    def ct_copy(d, k, slot):
        return pltpu.make_async_copy(ct.at[slot], c_ref.at[:, cols(d * NT + k)], ct_sem.at[slot])

    ra_start(0, 0, 0)

    def own_work(t, d, k, slot):
        @pl.when(t < last)
        def _():
            ra_start(1 - d, (t + 1) // 2, 1 - slot)

        ra_copy(d, k, slot).wait()
        mine = jnp.dot(af[y], bt[slot], preferred_element_type=F32) + rat[slot]
        rat[slot] = mine
        c_copy(d, k).wait_recv()

        @pl.when(t >= 2)
        def _():
            ct_copy(d, k, slot).wait()

        ct[slot] = (rat[slot] + rc[d, k]).astype(ct.dtype)
        ct_copy(d, k, slot).start()

    run(tile_b, None, own_work)
    for d in range(2):
        ct_copy(d, NT - 1, d).wait()

    for d in (1, 2, 3):
        s1_copy(d).wait_send()
    for r in range(1, ny):
        s2_piece(r, False)
    for m in range(ny):
        for side in range(2):
            s3_copy(m, side).wait_send()
            s4_copy(m, side).wait_send()

    def drain(t, _):
        bx_copy(t).wait_send()
        b_copy(lax.rem(t, 2), t // 2).wait_send()
        c_copy(lax.rem(t, 2), t // 2).wait_send()
        return 0

    lax.fori_loop(0, 2 * NT, drain, 0)


def solution(mesh):
    grid_spec = P(("dp", "ri", "ro"), "co")
    ny, nx = mesh.shape["ri"], mesh.shape["co"]

    def local_block(a, b):
        rows, depth = a.shape
        kh, width = b.shape
        w = width // (2 * NT)
        q = rows // nx
        any_spec = pl.BlockSpec(memory_space=pl.ANY)
        dma = pltpu.SemaphoreType.DMA
        out = pl.pallas_call(
            functools.partial(kernel, ny, nx),
            out_shape=[
                jax.ShapeDtypeStruct((rows, width), jnp.bfloat16),
                jax.ShapeDtypeStruct((kh, width), b.dtype),
                jax.ShapeDtypeStruct((nx, q, depth), a.dtype),
                jax.ShapeDtypeStruct((2, NT, rows, w), F32),
            ],
            in_specs=[any_spec] * 2,
            out_specs=[any_spec] * 4,
            scratch_shapes=[
                pltpu.VMEM((ny, rows, depth), a.dtype),
                pltpu.VMEM((2, 2 * kh, w), b.dtype),
                pltpu.VMEM((2, NT, rows, w), F32),
                pltpu.VMEM((2, NT, rows, w), F32),
                pltpu.VMEM((2, NT, rows, w), F32),
                pltpu.VMEM((2, NT, rows, w), F32),
                pltpu.VMEM((2, rows, w), F32),
                pltpu.VMEM((2, rows, w), jnp.bfloat16),
                dma((2 * NT,)), dma((2 * NT,)), dma((2, 2)),
                dma((nx,)), dma((nx,)), dma((ny,)), dma((ny,)),
                dma((ny, 2)), dma((ny, 2)), dma((ny, 2)), dma((ny, 2)),
                dma((2, NT, nx)), dma((2, NT, nx)),
                dma((2, NT)), dma((2, NT)), dma((2, NT)), dma((2, NT)),
                dma((2,)), dma((2,)),
            ],
            compiler_params=pltpu.CompilerParams(
                collective_id=0, has_side_effects=True, vmem_limit_bytes=67043328
            ),
        )(a, b)
        return out[0]

    return jax.shard_map(local_block, mesh=mesh, in_specs=(grid_spec, grid_spec), out_specs=grid_spec, check_vma=False)
```

```python
import functools

import jax
import jax.numpy as jnp
from jax import lax
from jax.experimental import pallas as pl
from jax.experimental.pallas import tpu as pltpu
from jax.sharding import PartitionSpec as P

MESH = pl.DeviceIdType.MESH
NT = 6
F32 = jnp.float32


def kernel(
    ny, nx, a_ref, b_ref, c_ref, bx, s1, f1, f2, ra,
    af, bt, sa, sb, rb, rc, rat, ct,
    bx_send, bx_recv, bt_sem, s1_send, s1_recv, d2_send, f1_send, f1_recv, s2_send, s2_recv, own_sem,
    s2b_send, f2_send, f2_recv, s3_send, s3_recv, s4_send, s4_recv,
    a_send, a_recv, b_send, b_recv, c_send, c_recv, ra_sem, ct_sem,
):
    y, x, core = lax.axis_index("ri"), lax.axis_index("co"), lax.axis_index("ro")
    rows = a_ref.shape[0]
    kh = b_ref.shape[0]
    w = b_ref.shape[1] // (2 * NT)
    q = rows // nx
    u = q // 3
    h = u // 2
    tiles = 2 * NT

    SUB = ((0, u), (u, 2 * u))
    A_ROWS = ((0, u), (u, 2 * u), (3 * u, 2 * u), (5 * u, 4 * u), (9 * u, 3 * u))
    B_ROWS = ((0, 3 * u), (3 * u, 9 * u))
    S3_AT = ((4 * u, 7 * u), (3 * u, 5 * u))
    S4 = ((0, 7 * u, 10 * u, 3 * h), (1, 3 * u, 9 * u, u), (1, 13 * h, 23 * h, h))
    OUT = ((0, 0, 0, 3 * u), (1, 0, 3 * u, u), (nx - 1, 0, 4 * u, u), (1, u, 5 * u, 2 * u),
           (nx - 1, u, 7 * u, 2 * u), (2, 0, 9 * u, 3 * u))

    def ym(d):
        return lax.rem(y + d + ny, ny)

    def xm(d):
        return lax.rem(x + d + nx, nx)

    def at_quarter(i, first, n):
        return pl.ds(pl.multiple_of(i * q + first, h), n)

    def rcopy(src, dst, ss, rs, **dev):
        return pltpu.make_async_remote_copy(
            src_ref=src, dst_ref=dst, send_sem=ss, recv_sem=rs, device_id=dev, device_id_type=MESH
        )

    barrier = pltpu.get_barrier_semaphore()
    for d in (1, nx - 1):
        pl.semaphore_signal(barrier, inc=1, device_id={"co": xm(d)}, device_id_type=MESH)
    for d in (1, ny - 1):
        pl.semaphore_signal(barrier, inc=1, device_id={"ri": ym(d)}, device_id_type=MESH)
    pl.semaphore_signal(barrier, inc=1, device_id={"ro": 1 - core}, device_id_type=MESH)
    pl.semaphore_wait(barrier, 5)

    odd = lax.rem(x + y, 2) == 1
    even = jnp.logical_not(odd)

    def split(piece, side):
        first, n = SUB[piece]
        return first + side * (n // 2), n // 2

    def f1_rows(piece):
        return pl.ds(piece * h, (piece + 1) * h)

    def d1_copy(side, piece):
        first, n = SUB[piece]
        return rcopy(
            a_ref.at[at_quarter(xm(1 - 2 * side), first, n)], s1.at[x, pl.ds(first, n)],
            s1_send.at[side, piece], s1_recv.at[x, piece, 0], co=xm(1 - 2 * side),
        )

    def d2_copy(side, piece):
        first, n = split(piece, side)
        return rcopy(
            a_ref.at[at_quarter(xm(2), first, n)], f1.at[side, f1_rows(piece)],
            d2_send.at[side, piece], f1_recv.at[side, piece], co=xm(1 - 2 * side),
        )

    def f1_copy(side, piece):
        first, n = split(piece, side)
        source = xm(2 * side - 1)
        return rcopy(
            f1.at[side, f1_rows(piece)], s1.at[source, pl.ds(first, n)],
            f1_send.at[side, piece], s1_recv.at[source, piece, side], co=xm(1 - 2 * side),
        )

    def s1_start():
        for piece in range(2):
            for make in (d2_copy, d1_copy):
                for side in range(2):
                    make(side, piece).start()

    def f1_relay(piece):
        for side in range(2):
            d2_copy(side, piece).wait_recv()
            f1_copy(side, piece).start()

    def s1_wait(r, piece):
        a = ym(r)

        @pl.when(lax.rem(a + x, 2) == 1)
        def _():
            first, n = SUB[piece]
            part = s1.at[a, pl.ds(first, n)]
            rcopy(part, part, s1_send.at[0, 0], s1_recv.at[a, piece, 0], co=x).wait_recv()

        @pl.when(a == xm(2))
        def _():
            for side in range(2):
                first, n = split(piece, side)
                part = s1.at[a, pl.ds(first, n)]
                rcopy(part, part, s1_send.at[0, 0], s1_recv.at[a, piece, side], co=x).wait_recv()

    def cols(tile):
        return pl.ds(pl.multiple_of(tile * w, w), w)

    def bx_copy(tile):
        return rcopy(b_ref.at[:, cols(tile)], bx.at[:, cols(tile)], bx_send.at[tile], bx_recv.at[tile], ro=1 - core)

    def tile_a(t):
        return (1 - lax.rem(t, 2)) * NT + t // 2

    def tile_b(t):
        return lax.rem(t, 2) * NT + t // 2

    def bt_copies(tile, slot):
        return (
            pltpu.make_async_copy(
                b_ref.at[:, cols(tile)], bt.at[slot, pl.ds(pl.multiple_of(core * kh, kh), kh)], bt_sem.at[slot, 0]
            ),
            pltpu.make_async_copy(
                bx.at[:, cols(tile)], bt.at[slot, pl.ds(pl.multiple_of((1 - core) * kh, kh), kh)], bt_sem.at[slot, 1]
            ),
        )

    def bt_start(tile, slot):
        for cp in bt_copies(tile, slot):
            cp.start()

    def bt_wait(tile, slot):
        for cp in bt_copies(tile, slot):
            cp.wait()

    def from_a(a, first, n, do):
        for src, cond in ((a_ref.at[at_quarter(x, first, n)], a == x), (s1.at[a, pl.ds(first, n)], a != x)):

            @pl.when(cond)
            def _(src=src):
                do(src)

    def s2_copy(r, piece, src):
        first, n = SUB[piece]
        return rcopy(src, af.at[y, pl.ds(first, n)], s2_send.at[r, piece], s2_recv.at[y, piece], ri=ym(r))

    def s2_wait(m, piece):
        first, n = SUB[piece]
        part = af.at[m, pl.ds(first, n)]
        rcopy(part, part, s2_send.at[1, 0], s2_recv.at[m, piece], ri=y).wait_recv()

    def s2_early(r):
        @pl.when(ym(r) == x)
        def _():
            for piece in range(2):
                first, n = SUB[piece]
                s2_copy(r, piece, a_ref.at[at_quarter(x, first, n)]).start()

    def s2_start(r, piece):
        s1_wait(r, piece)

        @pl.when(ym(r) != x)
        def _():
            first, n = SUB[piece]
            s2_copy(r, piece, s1.at[ym(r), pl.ds(first, n)]).start()

    def s2b_start():
        for side in range(2):
            from_a(
                ym(2), side * 3 * h, 3 * h,
                lambda src, side=side: rcopy(
                    src, f2.at[side], s2b_send.at[side], f2_recv.at[side], ri=ym(1 - 2 * side)
                ).start(),
            )

    def f2_copy(side):
        m = ym(2 * side - 1)
        return rcopy(
            f2.at[side], af.at[m, pl.ds(side * 3 * h, 3 * h)], f2_send.at[side], s2_recv.at[m, side], ri=ym(1 - 2 * side)
        )

    def f2_relay():
        for side in range(2):
            rcopy(f2.at[side], f2.at[side], s2b_send.at[side], f2_recv.at[side], ri=y).wait_recv()
            f2_copy(side).start()

    def f2_wait():
        m = ym(2)
        for side in range(2):
            part = af.at[m, pl.ds(side * 3 * h, 3 * h)]
            rcopy(part, part, f2_send.at[side], s2_recv.at[m, side], ri=y).wait_recv()

    def own_copy(src):
        return pltpu.make_async_copy(src, af.at[y, pl.ds(0, q)], own_sem)

    def s3_copy(m, side, piece):
        first, n = SUB[piece]
        return rcopy(
            af.at[m, pl.ds(first, n)], af.at[m, pl.ds(S3_AT[side][piece], n)],
            s3_send.at[m, side, piece], s3_recv.at[m, side, piece], co=xm(1 - 2 * side),
        )

    def s3_start(m, piece):
        for side in range(2):
            s3_copy(m, side, piece).start()

    def s3_wait(m, piece):
        for side in range(2):
            s3_copy(m, side, piece).wait_recv()

    def s4_copy(m, i):
        side, src, dst, n = S4[i]
        return rcopy(
            af.at[m, pl.ds(src, n)], af.at[m, pl.ds(dst, n)], s4_send.at[m, i], s4_recv.at[m, i], co=xm(1 - 2 * side)
        )

    def s4_start(m):
        for i in range(3):
            s4_copy(m, i).start()

    def s4_wait(m):
        for i in range(3):
            s4_copy(m, i).wait_recv()

    near = (1, ny - 1)

    @pl.when(odd)
    def _():
        s1_start()

    for r in near:
        s2_early(r)

    def bx_start(t, _):
        bx_copy(tile_a(t)).start()
        return 0

    lax.fori_loop(0, tiles, bx_start, 0)

    @pl.when(even)
    def _():
        f1_relay(0)

    for r in near:
        s2_start(r, 0)

    @pl.when(even)
    def _():
        f1_relay(1)
        s1_start()

    for t in range(2):
        bx_copy(tile_a(t)).wait_recv()
        bt_start(tile_a(t), t)
    for r in near:
        s2_wait(ym(r), 0)
        s3_start(ym(r), 0)

    def dest(d):
        return lax.rem(y + 1 + d * (ny - 2), ny)

    def a_copy(d, k, i):
        part = pl.ds(*A_ROWS[i])
        return rcopy(sa.at[d, k, part], ra.at[d, k, part], a_send.at[d, k, i], a_recv.at[d, k, i], ri=dest(d))

    def b_copy(d, k, i):
        part = pl.ds(*B_ROWS[i])
        return rcopy(sb.at[d, k, part], rb.at[d, k, part], b_send.at[d, k, i], b_recv.at[d, k, i], ri=dest(d))

    def c_copy(d, k):
        return rcopy(sa.at[d, k], rc.at[d, k], c_send.at[d, k], c_recv.at[d, k], ri=dest(d))

    def run(this, nxt, work, each=None):
        def step(t, carry):
            if each is not None:
                each(t)

            @pl.when(t + 2 < tiles)
            def _():
                bt_start(this(t + 2), lax.rem(t + 2, 3))

            if nxt is not None:

                @pl.when(t + 2 >= tiles)
                def _():
                    bt_start(nxt(t + 2 - tiles), lax.rem(t + 2, 3))

            slot = lax.rem(t, 3)
            bt_wait(this(t), slot)
            work(t, lax.rem(t, 2), t // 2, slot)
            return carry

        lax.fori_loop(0, tiles, step, 0)

    def a_pass(i, nxt, each=None):
        part = pl.ds(*A_ROWS[i])

        def work(t, d, k, slot):
            sa[d, k, part] = jnp.dot(af[dest(d), part], bt[slot], preferred_element_type=F32)
            a_copy(d, k, i).start()

        run(tile_a, nxt, work, each)

    def first_pass(t):
        @pl.when(t + 2 < tiles)
        def _():
            bx_copy(tile_a(t + 2)).wait_recv()

        @pl.when(t == NT)
        def _():
            for r in near:
                s2_start(r, 1)

    a_pass(0, tile_a, first_pass)
    for r in near:
        s2_wait(ym(r), 1)
        s3_start(ym(r), 1)
    a_pass(1, tile_a)

    @pl.when(odd)
    def _():
        f1_relay(0)
        f1_relay(1)

    for r in near:
        s3_wait(ym(r), 0)
    a_pass(2, tile_a)
    for piece in range(2):
        s1_wait(2, piece)
    s2b_start()
    for r in near:
        s3_wait(ym(r), 1)
        s4_start(ym(r))
    a_pass(3, tile_a)
    f2_relay()
    for r in near:
        s4_wait(ym(r))
    a_pass(4, tile_b)
    f2_wait()
    for piece in range(2):
        s3_start(ym(2), piece)
        s1_wait(0, piece)
    from_a(y, 0, q, lambda src: own_copy(src).start())

    def b_pass(i, nxt):
        part = pl.ds(*B_ROWS[i])

        def work(t, d, k, slot):
            sb[d, k, part] = jnp.dot(af[ym(2), part], bt[slot], preferred_element_type=F32)
            b_copy(d, k, i).start()

        run(tile_b, nxt, work)

    b_pass(0, tile_b)
    for piece in range(2):
        s3_wait(ym(2), piece)
    s4_start(ym(2))
    from_a(y, 0, q, lambda src: own_copy(src).wait())
    for piece in range(2):
        s3_start(y, piece)
    s4_wait(ym(2))
    b_pass(1, tile_b)
    for piece in range(2):
        s3_wait(y, piece)
    s4_start(y)

    def c_work(t, d, k, slot):
        for i in range(len(A_ROWS)):
            a_copy(d, k, i).wait_send()
        for i in range(len(B_ROWS)):
            b_copy(d, k, i).wait_recv()
        sa[d, k] = jnp.dot(af[dest(d)], bt[slot], preferred_element_type=F32) + rb[d, k]
        c_copy(d, k).start()

    run(tile_b, tile_b, c_work)
    s4_wait(y)

    def ra_copy(d, k, slot):
        return pltpu.make_async_copy(ra.at[1 - d, k], rat.at[slot], ra_sem.at[slot])

    def ra_start(d, k, slot):
        for i in range(len(A_ROWS)):
            a_copy(1 - d, k, i).wait_recv()
        ra_copy(d, k, slot).start()

    def ct_copies(d, k, slot):
        return [
            pltpu.make_async_copy(
                ct.at[slot, pl.ds(src, n)], c_ref.at[at_quarter(xm(j), first, n), cols(d * NT + k)], ct_sem.at[slot, i]
            )
            for i, (j, first, src, n) in enumerate(OUT)
        ]

    ra_start(0, 0, 0)

    def own_work(t, d, k, slot):
        @pl.when(t < tiles - 1)
        def _():
            ra_start(1 - d, (t + 1) // 2, 1 - d)

        ra_copy(d, k, d).wait()
        rat[d] = jnp.dot(af[y], bt[slot], preferred_element_type=F32) + rat[d]
        c_copy(d, k).wait_recv()

        @pl.when(t >= 2)
        def _():
            for cp in ct_copies(d, k, d):
                cp.wait()

        ct[d] = (rat[d] + rc[d, k]).astype(ct.dtype)
        for cp in ct_copies(d, k, d):
            cp.start()

    run(tile_b, None, own_work)
    for d in range(2):
        for cp in ct_copies(d, NT - 1, d):
            cp.wait()

    for side in range(2):
        for piece in range(2):
            for make in (d1_copy, d2_copy, f1_copy):
                make(side, piece).wait_send()
        rcopy(f2.at[side], f2.at[side], s2b_send.at[side], f2_recv.at[side], ri=y).wait_send()
        f2_copy(side).wait_send()
    for piece in range(2):
        for r in near:
            first, n = SUB[piece]
            s2_copy(r, piece, s1.at[y, pl.ds(first, n)]).wait_send()
    for m in range(ny):
        for side in range(2):
            for piece in range(2):
                s3_copy(m, side, piece).wait_send()
        for i in range(3):
            s4_copy(m, i).wait_send()

    def drain(t, _):
        d, k = lax.rem(t, 2), t // 2
        bx_copy(t).wait_send()
        for i in range(len(B_ROWS)):
            b_copy(d, k, i).wait_send()
        c_copy(d, k).wait_send()
        return 0

    lax.fori_loop(0, tiles, drain, 0)


def solution(mesh):
    grid_spec = P(("dp", "ri", "ro"), "co")
    ny, nx = mesh.shape["ri"], mesh.shape["co"]

    def local_block(a, b):
        rows, depth = a.shape
        kh, width = b.shape
        w = width // (2 * NT)
        q = rows // nx
        any_spec = pl.BlockSpec(memory_space=pl.ANY)
        dma = pltpu.SemaphoreType.DMA
        out = pl.pallas_call(
            functools.partial(kernel, ny, nx),
            out_shape=[
                jax.ShapeDtypeStruct((rows, width), jnp.bfloat16),
                jax.ShapeDtypeStruct((kh, width), b.dtype),
                jax.ShapeDtypeStruct((nx, q, depth), a.dtype),
                jax.ShapeDtypeStruct((2, q // 2, depth), a.dtype),
                jax.ShapeDtypeStruct((2, q // 2, depth), a.dtype),
                jax.ShapeDtypeStruct((2, NT, rows, w), F32),
            ],
            in_specs=[any_spec] * 2,
            out_specs=[any_spec] * 6,
            scratch_shapes=[
                pltpu.VMEM((ny, rows, depth), a.dtype),
                pltpu.VMEM((3, 2 * kh, w), b.dtype),
                pltpu.VMEM((2, NT, rows, w), F32),
                pltpu.VMEM((2, NT, rows, w), F32),
                pltpu.VMEM((2, NT, rows, w), F32),
                pltpu.VMEM((2, NT, rows, w), F32),
                pltpu.VMEM((2, rows, w), F32),
                pltpu.VMEM((2, rows, w), jnp.bfloat16),
                dma((2 * NT,)), dma((2 * NT,)), dma((3, 2)),
                dma((2, 2)), dma((nx, 2, 2)), dma((2, 2)), dma((2, 2)), dma((2, 2)), dma((ny, 2)), dma((ny, 2)), dma,
                dma((2,)), dma((2,)), dma((2,)), dma((ny, 2, 2)), dma((ny, 2, 2)), dma((ny, 3)), dma((ny, 3)),
                dma((2, NT, 5)), dma((2, NT, 5)), dma((2, NT, 2)), dma((2, NT, 2)), dma((2, NT)), dma((2, NT)),
                dma((2,)), dma((2, 6)),
            ],
            compiler_params=pltpu.CompilerParams(
                collective_id=0, has_side_effects=True, vmem_limit_bytes=67043328
            ),
        )(a, b)
        return out[0]

    return jax.shard_map(local_block, mesh=mesh, in_specs=(grid_spec, grid_spec), out_specs=grid_spec, check_vma=False)
```

```python
import functools

import jax
import jax.numpy as jnp
from jax import lax
from jax.experimental import pallas as pl
from jax.experimental.pallas import tpu as pltpu
from jax.sharding import PartitionSpec as P

MESH = pl.DeviceIdType.MESH
NT = 6
KC = 4
F32 = jnp.float32


def kernel(
    ny, nx, a_ref, b_ref, c_ref, bx, s1, f1, f2, ra,
    af, bt, sa, sb, rb, rc, rat, ct,
    bx_send, bx_recv, bt_sem, s1_send, s1_recv, d2_send, f1_send, f1_recv, s2_send, s2_recv, own_sem,
    s2b_send, f2_send, f2_recv, s3_send, s3_recv, s4_send, s4_recv,
    a_send, a_recv, b_send, b_recv, c_send, c_recv, ra_sem, ct_sem,
):
    y, x, core = lax.axis_index("ri"), lax.axis_index("co"), lax.axis_index("ro")
    rows = a_ref.shape[0]
    kh = b_ref.shape[0]
    w = b_ref.shape[1] // (2 * NT)
    q = rows // nx
    u = q // 2
    h = u // 2
    kw = a_ref.shape[1] // KC
    tiles = 2 * NT

    def sub(piece):
        return pl.ds(piece * u, u)

    A_ROWS = ((0, u), (u, u), (2 * u, 2 * u), (4 * u, 2 * u), (6 * u, 2 * u))
    B_ROWS = ((0, 2 * u), (2 * u, 6 * u))
    S3_AT = ((3 * u, 5 * u), (2 * u, 4 * u))
    S4 = ((0, 5 * u, 7 * u), (1, 2 * u, 6 * u))
    OUT = ((0, 0, 0, 2 * u), (1, 0, 2 * u, u), (nx - 1, 0, 3 * u, u), (1, u, 4 * u, u),
           (nx - 1, u, 5 * u, u), (2, 0, 6 * u, 2 * u))

    def ym(d):
        return lax.rem(y + d + ny, ny)

    def xm(d):
        return lax.rem(x + d + nx, nx)

    def at_quarter(i, first, n):
        return pl.ds(pl.multiple_of(i * q + first, h), n)

    def rcopy(src, dst, ss, rs, **dev):
        return pltpu.make_async_remote_copy(
            src_ref=src, dst_ref=dst, send_sem=ss, recv_sem=rs, device_id=dev, device_id_type=MESH
        )

    barrier = pltpu.get_barrier_semaphore()
    for d in (1, nx - 1):
        pl.semaphore_signal(barrier, inc=1, device_id={"co": xm(d)}, device_id_type=MESH)
    for d in (1, ny - 1):
        pl.semaphore_signal(barrier, inc=1, device_id={"ri": ym(d)}, device_id_type=MESH)
    pl.semaphore_signal(barrier, inc=1, device_id={"ro": 1 - core}, device_id_type=MESH)
    pl.semaphore_wait(barrier, 5)

    odd = lax.rem(x + y, 2) == 1
    even = jnp.logical_not(odd)

    def piece_of(chunk):
        return (1, slice(None)) if chunk == KC else (0, pl.ds(chunk * kw, kw))

    def s1_part(a, chunk):
        piece, at = piece_of(chunk)
        return s1.at[a, sub(piece), at]

    def s1_half(a, chunk, side):
        piece, at = piece_of(chunk)
        return s1.at[a, pl.ds(piece * u + side * h, h), at]

    def f1_part(side, chunk):
        piece, at = piece_of(chunk)
        return f1.at[side, pl.ds(piece * h, h), at]

    def d1_copy(side, chunk):
        piece, at = piece_of(chunk)
        return rcopy(
            a_ref.at[at_quarter(xm(1 - 2 * side), piece * u, u), at], s1_part(x, chunk),
            s1_send.at[side, chunk], s1_recv.at[x, chunk, 0], co=xm(1 - 2 * side),
        )

    def d2_copy(side, chunk):
        piece, at = piece_of(chunk)
        return rcopy(
            a_ref.at[at_quarter(xm(2), piece * u + side * h, h), at], f1_part(side, chunk),
            d2_send.at[side, chunk], f1_recv.at[side, chunk], co=xm(1 - 2 * side),
        )

    def f1_copy(side, chunk):
        source = xm(2 * side - 1)
        return rcopy(
            f1_part(side, chunk), s1_half(source, chunk, side),
            f1_send.at[side, chunk], s1_recv.at[source, chunk, side], co=xm(1 - 2 * side),
        )

    def both(make, chunk):
        for side in range(2):
            make(side, chunk).start()

    def f1_relay(chunk):
        for side in range(2):
            d2_copy(side, chunk).wait_recv()
            f1_copy(side, chunk).start()

    def s1_wait(r, chunk):
        a = ym(r)

        @pl.when(lax.rem(a + x, 2) == 1)
        def _():
            part = s1_part(a, chunk)
            rcopy(part, part, s1_send.at[0, 0], s1_recv.at[a, chunk, 0], co=x).wait_recv()

        @pl.when(a == xm(2))
        def _():
            for side in range(2):
                part = s1_half(a, chunk, side)
                rcopy(part, part, s1_send.at[0, 0], s1_recv.at[a, chunk, side], co=x).wait_recv()

    def cols(tile):
        return pl.ds(pl.multiple_of(tile * w, w), w)

    def bx_copy(tile):
        return rcopy(b_ref.at[:, cols(tile)], bx.at[:, cols(tile)], bx_send.at[tile], bx_recv.at[tile], ro=1 - core)

    def tile_a(t):
        return (1 - lax.rem(t, 2)) * NT + t // 2

    def tile_b(t):
        return lax.rem(t, 2) * NT + t // 2

    def bt_copies(tile, slot):
        return (
            pltpu.make_async_copy(
                b_ref.at[:, cols(tile)], bt.at[slot, pl.ds(pl.multiple_of(core * kh, kh), kh)], bt_sem.at[slot, 0]
            ),
            pltpu.make_async_copy(
                bx.at[:, cols(tile)], bt.at[slot, pl.ds(pl.multiple_of((1 - core) * kh, kh), kh)], bt_sem.at[slot, 1]
            ),
        )

    def bt_start(tile, slot):
        for cp in bt_copies(tile, slot):
            cp.start()

    def bt_wait(tile, slot):
        for cp in bt_copies(tile, slot):
            cp.wait()

    def from_a(a, first, n, do):
        for src, cond in ((a_ref.at[at_quarter(x, first, n)], a == x), (s1.at[a, pl.ds(first, n)], a != x)):

            @pl.when(cond)
            def _(src=src):
                do(src)

    def s2_copy(r, chunk, src):
        piece, at = piece_of(chunk)
        return rcopy(src, af.at[y, sub(piece), at], s2_send.at[r, chunk], s2_recv.at[y, chunk], ri=ym(r))

    def s2_wait(m, chunk):
        piece, at = piece_of(chunk)
        part = af.at[m, sub(piece), at]
        rcopy(part, part, s2_send.at[1, 0], s2_recv.at[m, chunk], ri=y).wait_recv()

    def s2_early(r):
        @pl.when(ym(r) == x)
        def _():
            for chunk in range(KC + 1):
                piece, at = piece_of(chunk)
                s2_copy(r, chunk, a_ref.at[at_quarter(x, piece * u, u), at]).start()

    def s2_start(r, chunk):
        s1_wait(r, chunk)

        @pl.when(ym(r) != x)
        def _():
            s2_copy(r, chunk, s1_part(ym(r), chunk)).start()

    def s2b_start():
        for side in range(2):
            from_a(
                ym(2), side * u, u,
                lambda src, side=side: rcopy(
                    src, f2.at[side], s2b_send.at[side], f2_recv.at[side], ri=ym(1 - 2 * side)
                ).start(),
            )

    def f2_copy(side):
        m = ym(2 * side - 1)
        return rcopy(f2.at[side], af.at[m, sub(side)], f2_send.at[side], s2_recv.at[m, side], ri=ym(1 - 2 * side))

    def f2_relay():
        for side in range(2):
            rcopy(f2.at[side], f2.at[side], s2b_send.at[side], f2_recv.at[side], ri=y).wait_recv()
            f2_copy(side).start()

    def f2_wait():
        m = ym(2)
        for side in range(2):
            part = af.at[m, sub(side)]
            rcopy(part, part, f2_send.at[side], s2_recv.at[m, side], ri=y).wait_recv()

    def own_copy(src):
        return pltpu.make_async_copy(src, af.at[y, pl.ds(0, q)], own_sem)

    def s3_copy(m, side, piece):
        return rcopy(
            af.at[m, sub(piece)], af.at[m, pl.ds(S3_AT[side][piece], u)],
            s3_send.at[m, side, piece], s3_recv.at[m, side, piece], co=xm(1 - 2 * side),
        )

    def s3_start(m, piece):
        for side in range(2):
            s3_copy(m, side, piece).start()

    def s3_wait(m, piece):
        for side in range(2):
            s3_copy(m, side, piece).wait_recv()

    def s4_copy(m, i):
        side, src, dst = S4[i]
        return rcopy(
            af.at[m, pl.ds(src, u)], af.at[m, pl.ds(dst, u)], s4_send.at[m, i], s4_recv.at[m, i], co=xm(1 - 2 * side)
        )

    def s4_start(m):
        for i in range(2):
            s4_copy(m, i).start()

    def s4_wait(m):
        for i in range(2):
            s4_copy(m, i).wait_recv()

    near = (1, ny - 1)

    @pl.when(odd)
    def _():
        for chunk in range(KC + 1):
            both(d2_copy, chunk)
            both(d1_copy, chunk)

    @pl.when(even)
    def _():
        for chunk in range(KC):
            both(d2_copy, chunk)

    for r in near:
        s2_early(r)

    def bx_start(t, _):
        bx_copy(tile_a(t)).start()
        return 0

    lax.fori_loop(0, tiles, bx_start, 0)

    for chunk in range(KC):

        @pl.when(even)
        def _(chunk=chunk):
            f1_relay(chunk)
            both(d1_copy, chunk)

        for r in near:
            s2_start(r, chunk)

    @pl.when(even)
    def _():
        f1_relay(KC)
        both(d2_copy, KC)
        both(d1_copy, KC)

    for t in range(2):
        bx_copy(tile_a(t)).wait_recv()
        bt_start(tile_a(t), t)
    for r in near:
        for chunk in range(KC):
            s2_wait(ym(r), chunk)
        s3_start(ym(r), 0)

    def dest(d):
        return lax.rem(y + 1 + d * (ny - 2), ny)

    def a_copy(d, k, i):
        part = pl.ds(*A_ROWS[i])
        return rcopy(sa.at[d, k, part], ra.at[d, k, part], a_send.at[d, k, i], a_recv.at[d, k, i], ri=dest(d))

    def b_copy(d, k, i):
        part = pl.ds(*B_ROWS[i])
        return rcopy(sb.at[d, k, part], rb.at[d, k, part], b_send.at[d, k, i], b_recv.at[d, k, i], ri=dest(d))

    def c_copy(d, k):
        return rcopy(sa.at[d, k], rc.at[d, k], c_send.at[d, k], c_recv.at[d, k], ri=dest(d))

    def run(this, nxt, work, each=None):
        def step(t, carry):
            if each is not None:
                each(t)

            @pl.when(t + 2 < tiles)
            def _():
                bt_start(this(t + 2), lax.rem(t + 2, 3))

            if nxt is not None:

                @pl.when(t + 2 >= tiles)
                def _():
                    bt_start(nxt(t + 2 - tiles), lax.rem(t + 2, 3))

            slot = lax.rem(t, 3)
            bt_wait(this(t), slot)
            work(t, lax.rem(t, 2), t // 2, slot)
            return carry

        lax.fori_loop(0, tiles, step, 0)

    def a_pass(i, nxt, each=None):
        part = pl.ds(*A_ROWS[i])

        def work(t, d, k, slot):
            sa[d, k, part] = jnp.dot(af[dest(d), part], bt[slot], preferred_element_type=F32)
            a_copy(d, k, i).start()

        run(tile_a, nxt, work, each)

    def first_pass(t):
        @pl.when(t + 2 < tiles)
        def _():
            bx_copy(tile_a(t + 2)).wait_recv()

        @pl.when(t == 4)
        def _():
            for r in near:
                s2_start(r, KC)

    a_pass(0, tile_a, first_pass)

    @pl.when(odd)
    def _():
        for chunk in range(KC + 1):
            f1_relay(chunk)

    for r in near:
        s2_wait(ym(r), KC)
        s3_start(ym(r), 1)
    a_pass(1, tile_a)
    for chunk in range(KC + 1):
        s1_wait(2, chunk)
    s2b_start()
    for r in near:
        s3_wait(ym(r), 0)
    a_pass(2, tile_a)
    f2_relay()
    for r in near:
        s3_wait(ym(r), 1)
        s4_start(ym(r))
    a_pass(3, tile_a)
    for r in near:
        s4_wait(ym(r))
    a_pass(4, tile_b)
    f2_wait()
    for piece in range(2):
        s3_start(ym(2), piece)
    for chunk in range(KC + 1):
        s1_wait(0, chunk)
    from_a(y, 0, q, lambda src: own_copy(src).start())

    def b_pass(i, nxt):
        part = pl.ds(*B_ROWS[i])

        def work(t, d, k, slot):
            sb[d, k, part] = jnp.dot(af[ym(2), part], bt[slot], preferred_element_type=F32)
            b_copy(d, k, i).start()

        run(tile_b, nxt, work)

    b_pass(0, tile_b)
    for piece in range(2):
        s3_wait(ym(2), piece)
    s4_start(ym(2))
    from_a(y, 0, q, lambda src: own_copy(src).wait())
    for piece in range(2):
        s3_start(y, piece)
    s4_wait(ym(2))
    b_pass(1, tile_b)
    for piece in range(2):
        s3_wait(y, piece)
    s4_start(y)

    def c_work(t, d, k, slot):
        for i in range(len(A_ROWS)):
            a_copy(d, k, i).wait_send()
        for i in range(len(B_ROWS)):
            b_copy(d, k, i).wait_recv()
        sa[d, k] = jnp.dot(af[dest(d)], bt[slot], preferred_element_type=F32) + rb[d, k]
        c_copy(d, k).start()

    run(tile_b, tile_b, c_work)
    s4_wait(y)

    def ra_copy(d, k, slot):
        return pltpu.make_async_copy(ra.at[1 - d, k], rat.at[slot], ra_sem.at[slot])

    def ra_start(d, k, slot):
        for i in range(len(A_ROWS)):
            a_copy(1 - d, k, i).wait_recv()
        ra_copy(d, k, slot).start()

    def ct_copies(d, k, slot):
        return [
            pltpu.make_async_copy(
                ct.at[slot, pl.ds(src, n)], c_ref.at[at_quarter(xm(j), first, n), cols(d * NT + k)], ct_sem.at[slot, i]
            )
            for i, (j, first, src, n) in enumerate(OUT)
        ]

    ra_start(0, 0, 0)

    def own_work(t, d, k, slot):
        @pl.when(t < tiles - 1)
        def _():
            ra_start(1 - d, (t + 1) // 2, 1 - d)

        ra_copy(d, k, d).wait()
        for i in range(len(B_ROWS)):
            b_copy(d, k, i).wait_send()
        sb[d, k] = jnp.dot(af[y], bt[slot], preferred_element_type=F32) + rat[d]

    run(tile_b, None, own_work)

    def last_work(t, _):
        d, k = lax.rem(t, 2), t // 2

        @pl.when(t >= 2)
        def _():
            for cp in ct_copies(d, k, d):
                cp.wait()

        c_copy(d, k).wait_recv()
        ct[d] = (sb[d, k] + rc[d, k]).astype(ct.dtype)
        for cp in ct_copies(d, k, d):
            cp.start()
        return 0

    lax.fori_loop(0, tiles, last_work, 0)
    for d in range(2):
        for cp in ct_copies(d, NT - 1, d):
            cp.wait()

    for side in range(2):
        for chunk in range(KC + 1):
            for make in (d1_copy, d2_copy, f1_copy):
                make(side, chunk).wait_send()
        rcopy(f2.at[side], f2.at[side], s2b_send.at[side], f2_recv.at[side], ri=y).wait_send()
        f2_copy(side).wait_send()
    for chunk in range(KC + 1):
        for r in near:
            s2_copy(r, chunk, s1_part(y, chunk)).wait_send()
    for m in range(ny):
        for side in range(2):
            for piece in range(2):
                s3_copy(m, side, piece).wait_send()
        for i in range(2):
            s4_copy(m, i).wait_send()

    def drain(t, _):
        bx_copy(t).wait_send()
        c_copy(lax.rem(t, 2), t // 2).wait_send()
        return 0

    lax.fori_loop(0, tiles, drain, 0)


def solution(mesh):
    grid_spec = P(("dp", "ri", "ro"), "co")
    ny, nx = mesh.shape["ri"], mesh.shape["co"]

    def local_block(a, b):
        rows, depth = a.shape
        kh, width = b.shape
        w = width // (2 * NT)
        q = rows // nx
        any_spec = pl.BlockSpec(memory_space=pl.ANY)
        dma = pltpu.SemaphoreType.DMA
        out = pl.pallas_call(
            functools.partial(kernel, ny, nx),
            out_shape=[
                jax.ShapeDtypeStruct((rows, width), jnp.bfloat16),
                jax.ShapeDtypeStruct((kh, width), b.dtype),
                jax.ShapeDtypeStruct((nx, q, depth), a.dtype),
                jax.ShapeDtypeStruct((2, q // 2, depth), a.dtype),
                jax.ShapeDtypeStruct((2, q // 2, depth), a.dtype),
                jax.ShapeDtypeStruct((2, NT, rows, w), F32),
            ],
            in_specs=[any_spec] * 2,
            out_specs=[any_spec] * 6,
            scratch_shapes=[
                pltpu.VMEM((ny, rows, depth), a.dtype),
                pltpu.VMEM((3, 2 * kh, w), b.dtype),
                pltpu.VMEM((2, NT, rows, w), F32),
                pltpu.VMEM((2, NT, rows, w), F32),
                pltpu.VMEM((2, NT, rows, w), F32),
                pltpu.VMEM((2, NT, rows, w), F32),
                pltpu.VMEM((2, rows, w), F32),
                pltpu.VMEM((2, rows, w), jnp.bfloat16),
                dma((2 * NT,)), dma((2 * NT,)), dma((3, 2)),
                dma((2, KC + 1)), dma((nx, KC + 1, 2)), dma((2, KC + 1)), dma((2, KC + 1)), dma((2, KC + 1)),
                dma((ny, KC + 1)), dma((ny, KC + 1)), dma,
                dma((2,)), dma((2,)), dma((2,)), dma((ny, 2, 2)), dma((ny, 2, 2)), dma((ny, 2)), dma((ny, 2)),
                dma((2, NT, 5)), dma((2, NT, 5)), dma((2, NT, 2)), dma((2, NT, 2)), dma((2, NT)), dma((2, NT)),
                dma((2,)), dma((2, 6)),
            ],
            compiler_params=pltpu.CompilerParams(
                collective_id=0, has_side_effects=True, vmem_limit_bytes=67043328
            ),
        )(a, b)
        return out[0]

    return jax.shard_map(local_block, mesh=mesh, in_specs=(grid_spec, grid_spec), out_specs=grid_spec, check_vma=False)
```
